32 devices in a mesh: space: 8 (over y, x, core), tm: 4 (over z).
Axes of the slice: x: 2, y: 2, z: 4, core: 2. Of those that a mesh axis runs over, the one named last changes fastest.
Arguments:
- vectors: bfloat16 [4, 2, 3, 96, 4096], P('tm', None, None, None, 'space'), may hold values from -6 to 6
- momenta: int32 [2, 3], replicated, may hold values from -3 to 3
- offsets: int32 [8, 3], replicated, may hold values from 0 to 56, as said below
Outputs:
- elementals: float32 [4, 96, 2, 18432], P(None, 'space')
The draws below stay inside these ranges and needn't reach their ends.
Inputs may be any that keep to these rules, and one draw needn't show every extreme that they name: `offsets`: each row is the corner of one block of 8 x 8 x 8 sites of the 64^3 lattice: its first two coordinates are multiples of 8, its third a multiple of 8; no two rows name the same block, so the blocks never intersect.
All inputs are finite; a program needn't handle non-finite values.
Results may differ from the reference program's by a relative error of at most 0.0055.
Values may be sent and summed in bfloat16 or wider, within the bound.
A program may use at most 128 MiB of HBM per device.

```python
import math
import jax
import jax.numpy as jnp
from jax import lax

NVEC = 96
MOMENTA = 2
LAT = 64
BRICK = 8
BRICK_Z = 8
SITES_DEV = 512
SITES = 4096
BRICKS = 8
TIME = 4
N_SPACE = 8


def draw_offsets(key, part):
    across = LAT // BRICK
    along = LAT // BRICK_Z
    chosen = jax.random.permutation(key, across * across * along)[:BRICKS].astype(jnp.int32)
    first = chosen // (across * along)
    second = chosen // along % across
    third = chosen % along
    return jnp.stack([first * BRICK, second * BRICK, third * BRICK_Z], axis=1).astype(jnp.int32)


def place_ends(array, own_key, smallest, largest):
    longest = array.shape.index(max(array.shape))
    spots = []
    for shift in (0, 1):
        where = [jax.random.randint(jax.random.fold_in(own_key, axis), (), 0, length) for axis, length in enumerate(array.shape)]
        where[longest] = (where[longest] + shift) % array.shape[longest]
        spots.append(tuple(where))
    return array.at[spots[0]].set(smallest).at[spots[1]].set(largest)


def level_of(own_key, extent, shards, low, high):
    loudness = 1.0
    for position, parts in shards:
        heights = jax.random.uniform(jax.random.fold_in(jax.random.fold_in(own_key, 6), position), (parts,), jnp.float32, low / len(shards), high / len(shards))
        loudness = loudness * jnp.repeat(jnp.exp(heights), extent[position] // parts).reshape((-1,) + (1,) * (len(extent) - 1 - position))
    return loudness


def bell_draw(own_key, extent, scale, reach, pieces=(), kind=jnp.bfloat16):
    result = jax.random.normal(own_key, extent, jnp.float32) * scale
    if len(pieces) > 0:
        result = level_of(own_key, extent, pieces, -0.22, 0.18) * result
    return jnp.clip(result, min=-reach, max=reach).astype(kind)


def setup_inputs(seed: int = 0) -> dict:
    arg_keys = jax.random.split(jax.random.key(seed), 4)
    return {
        "vectors": bell_draw(arg_keys[0], (TIME, 2, 3, NVEC, SITES), 1.0, 6.0, ((0, 4), (4, 8))),
        "momenta": place_ends(jax.random.randint(arg_keys[1], (MOMENTA, 3), -3, 4), jax.random.fold_in(arg_keys[1], 1), -3, 3).astype(jnp.int32),
        "offsets": draw_offsets(jax.random.fold_in(arg_keys[3], 71), 0),
    }


def local_coords(site):
    return jnp.stack([site // (BRICK * BRICK_Z), site // BRICK_Z % BRICK, site % BRICK_Z])

def phases(momenta, coords):
    product = lax.optimization_barrier(jnp.sum(momenta[:, :, None] * coords[None, :, :], axis=1))
    angle = (product % LAT).astype(jnp.float32) * (2.0 * math.pi / LAT)
    return jnp.stack([jnp.cos(angle), jnp.sin(angle)], axis=1).astype(jnp.float32)

def complex_term(w_real, w_imag, v_real, v_imag):
    return (w_real * v_real - w_imag * v_imag, w_real * v_imag + w_imag * v_real)

def cross_rows(phase, row_vecs, vecs):
    phase_f = phase.astype(jnp.float32)
    rows_f = row_vecs.astype(jnp.float32)
    cosine = phase_f[:, 0][:, None, None, :]
    sine = phase_f[:, 1][:, None, None, :]
    real_w = cosine * rows_f[0][None] - sine * rows_f[1][None]
    imag_w = cosine * rows_f[1][None] + sine * rows_f[0][None]
    real_w = jnp.transpose(real_w, (2, 0, 1, 3))
    imag_w = jnp.transpose(imag_w, (2, 0, 1, 3))
    real_v = vecs[0].astype(jnp.float32)
    imag_v = vecs[1].astype(jnp.float32)
    real_parts = []
    imag_parts = []
    for colour in range(3):
        first = (colour + 1) % 3
        second = (colour + 2) % 3
        plus_re, plus_im = complex_term(real_w[:, :, first, None, :], imag_w[:, :, first, None, :], real_v[second][None, None], imag_v[second][None, None])
        minus_re, minus_im = complex_term(real_w[:, :, second, None, :], imag_w[:, :, second, None, :], real_v[first][None, None], imag_v[first][None, None])
        real_parts.append(plus_re - minus_re)
        imag_parts.append(plus_im - minus_im)
    stacked = jnp.stack([jnp.stack(real_parts, axis=3), jnp.stack(imag_parts, axis=3)], axis=3)
    return stacked.astype(jnp.bfloat16)

def mixing(vecs):
    real_v = vecs[0]
    imag_v = vecs[1]
    return jnp.stack([jnp.stack([real_v, imag_v], axis=1), jnp.stack([-imag_v, real_v], axis=1)])

def reference(vectors, momenta, offsets):
    site = jnp.arange(SITES, dtype=jnp.int32)
    brick_of = site // SITES_DEV
    coords = local_coords(site % SITES_DEV) + jnp.transpose(offsets[brick_of])
    phase = phases(momenta, coords)
    rows = NVEC // N_SPACE
    scale = 1.0 / math.sqrt(SITES)

    def one_time(slab):

        def one_block(index):
            first_row = index * rows

            def add(total, shard):
                begin = shard * SITES_DEV
                phase_part = lax.dynamic_slice_in_dim(phase, begin, SITES_DEV, 2)
                vec_part = lax.dynamic_slice_in_dim(slab, begin, SITES_DEV, 3)
                row_vecs = lax.dynamic_slice_in_dim(vec_part, first_row, rows, 2)
                crossed = cross_rows(phase_part, row_vecs, vec_part).astype(jnp.float32)
                operand = mixing(vec_part).astype(jnp.float32)
                part = jnp.einsum('imjqcg,qcrkg->imjrk', crossed, operand, precision=lax.Precision.HIGHEST)
                return (total + part, None)
            empty = jnp.zeros((rows, MOMENTA, NVEC, 2, NVEC), jnp.float32)
            total, unused = lax.scan(add, empty, jnp.arange(N_SPACE, dtype=jnp.int32))
            return (total * scale).reshape(rows, MOMENTA, 2 * NVEC * NVEC)
        blocks = lax.map(one_block, jnp.arange(N_SPACE, dtype=jnp.int32))
        return blocks.reshape(NVEC, MOMENTA, 2 * NVEC * NVEC)
    return lax.map(one_time, vectors)
```

```python
import functools
import math

import jax
import jax.numpy as jnp
from jax import lax
from jax.experimental import pallas as pl
from jax.experimental.pallas import tpu as pltpu
from jax.sharding import PartitionSpec as P

LAT = 64
BRICK = 8
BRICK_Z = 8
JB = 32
LANES = 128


def local_coords(site):
    return jnp.stack([site // (BRICK * BRICK_Z), site // BRICK_Z % BRICK, site % BRICK_Z])


def phases(momenta, coords):
    product = jnp.sum(momenta[:, :, None] * coords[None, :, :], axis=1)
    angle = (product % LAT).astype(jnp.float32) * (2.0 * math.pi / LAT)
    return jnp.stack([jnp.cos(angle), jnp.sin(angle)], axis=1)


def compute_kernel(scale, first, seeded, v_ref, row_ref, phase_ref, *refs):
    nvec = v_ref.shape[3]
    sites = v_ref.shape[4]
    rows = row_ref.shape[3]
    moments = phase_ref.shape[1] // 2
    nblocks = nvec // JB
    group = 2 * moments * JB
    if seeded:
        seed_ref, out_ref, row_f, vp_ref = refs[0], refs[1], refs[2], refs[3]
        rest = refs[4:]
        count = len(rest) // 2
        lhs_refs, acc_refs = rest[:count], rest[count:]
    else:
        acc_out, row_f, vp_ref = refs[0], refs[1], refs[2]
        lhs_refs = refs[3:]
        count = len(lhs_refs)
        starts = []
        at = 0
        for n in range(count):
            starts.append(at)
            at += (nblocks - first - n) * group
        acc_refs = [
            acc_out.at[:, pl.ds(starts[n], (nblocks - first - n) * group)] for n in range(count)
        ]
    step = pl.program_id(0)

    @pl.when(step == 0)
    def _():
        at = 0
        for acc in acc_refs:
            wide = acc.shape[1]
            if seeded:
                acc[...] = seed_ref[:, at : at + wide]
            else:
                acc[...] = jnp.zeros(acc.shape, jnp.float32)
            at += wide

    for q in range(2):
        for colour in range(3):
            row_f[q * 3 + colour] = row_ref[0, q, colour].astype(jnp.float32)

    def chunk(index, carry):
        lanes = pl.ds(pl.multiple_of(index * LANES, LANES), LANES)
        for colour in range(3):
            real_v = v_ref[0, 0, colour, :, lanes].astype(jnp.float32)
            imag_v = v_ref[0, 1, colour, :, lanes].astype(jnp.float32)
            for p in range(moments):
                cosine = phase_ref[0, pl.ds(2 * p, 1), lanes]
                sine = phase_ref[0, pl.ds(2 * p + 1, 1), lanes]
                real_x = (cosine * real_v - sine * imag_v).astype(jnp.bfloat16)
                imag_x = (cosine * imag_v + sine * real_v).astype(jnp.bfloat16)
                table = ((real_x, -imag_x), (imag_x, real_x))
                for r in range(2):
                    for q in range(2):
                        at = (colour * 2 + q) * LANES
                        for kb in range(first, nblocks):
                            base = (kb - first) * group + (2 * p + r) * JB
                            vp_ref[base : base + JB, at : at + LANES] = table[r][q][
                                kb * JB : (kb + 1) * JB
                            ]
        for n in range(count):
            jb = first + n
            vecs = [
                [v_ref[0, q, colour, jb * JB : (jb + 1) * JB, lanes] for colour in range(3)]
                for q in range(2)
            ]
            for i in range(rows):
                row = [
                    [
                        jnp.broadcast_to(
                            row_f[q * 3 + colour, pl.ds(i, 1), lanes], (JB, LANES)
                        ).astype(jnp.bfloat16)
                        for colour in range(3)
                    ]
                    for q in range(2)
                ]
                for colour in range(3):
                    a = (colour + 1) % 3
                    b = (colour + 2) % 3
                    real_d = (row[0][a] * vecs[0][b] - row[1][a] * vecs[1][b]) - (
                        row[0][b] * vecs[0][a] - row[1][b] * vecs[1][a]
                    )
                    imag_d = (row[0][a] * vecs[1][b] + row[1][a] * vecs[0][b]) - (
                        row[0][b] * vecs[1][a] + row[1][b] * vecs[0][a]
                    )
                    at = colour * 2 * LANES
                    lhs_refs[n][i * JB : (i + 1) * JB, at : at + LANES] = real_d
                    lhs_refs[n][i * JB : (i + 1) * JB, at + LANES : at + 2 * LANES] = imag_d
            acc_refs[n][...] += lax.dot_general(
                lhs_refs[n][...],
                vp_ref[n * group :, :],
                (((1,), (1,)), ((), ())),
                preferred_element_type=jnp.float32,
            )
        return carry

    lax.fori_loop(0, sites // LANES, chunk, 0)

    if seeded:

        @pl.when(step == pl.num_programs(0) - 1)
        def _():
            at = 0
            for acc in acc_refs:
                wide = acc.shape[1]
                out_ref[:, at : at + wide] = (acc[...] * scale).astype(jnp.bfloat16)
                at += wide


def contract(gathered, row_vecs, phase, scale, first, last, seed, seed_block):
    groups, _, _, nvec, sites = gathered.shape
    rows = row_vecs.shape[3]
    moments = phase.shape[1] // 2
    nblocks = nvec // JB
    group = 2 * moments * JB
    widths = [(nblocks - jb) * group for jb in range(first, last)]
    total = sum(widths)
    depth = 6 * LANES
    seeded = seed is not None
    in_specs = [
        pl.BlockSpec((1, 2, 3, nvec, sites), lambda s: (s, 0, 0, 0, 0)),
        pl.BlockSpec((1, 2, 3, rows, sites), lambda s: (s, 0, 0, 0, 0)),
        pl.BlockSpec((1, 2 * moments, sites), lambda s: (s, 0, 0)),
    ]
    operands = [gathered, row_vecs, phase]
    scratch = [
        pltpu.VMEM((6, rows, sites), jnp.float32),
        pltpu.VMEM((widths[0], depth), jnp.bfloat16),
    ] + [pltpu.VMEM((rows * JB, depth), jnp.bfloat16) for _ in widths]
    if seeded:
        in_specs.append(pl.BlockSpec((rows * JB, total), lambda s: (0, seed_block)))
        operands.append(seed)
        scratch += [pltpu.VMEM((rows * JB, wide), jnp.float32) for wide in widths]
    return pl.pallas_call(
        functools.partial(compute_kernel, scale, first, seeded),
        out_shape=jax.ShapeDtypeStruct(
            (rows * JB, total), jnp.bfloat16 if seeded else jnp.float32
        ),
        grid=(groups,),
        in_specs=in_specs,
        out_specs=pl.BlockSpec((rows * JB, total), lambda s: (0, 0)),
        scratch_shapes=scratch,
        compiler_params=pltpu.CompilerParams(dimension_semantics=("arbitrary",)),
        cost_estimate=pl.CostEstimate(
            flops=2 * groups * sites * 6 * rows * JB * total * 2,
            bytes_accessed=groups * 6 * nvec * sites * 2,
            transcendentals=0,
        ),
        name="contract",
    )(*operands)


def unpack_kernel(rows, moments, nvec, *refs):
    nblocks = nvec // JB
    group = 2 * moments * JB
    pack = LANES // JB
    head_ref, tail_ref, out_ref, full = refs
    tall = full.shape[0] // (rows * moments)
    pieces = []
    for n in range(nblocks):
        source = head_ref if n == 0 else tail_ref
        at = 0 if n == 0 else sum((nblocks - m) * group for m in range(1, n))
        for kb in range(n, nblocks):
            pieces.append((n, kb, source, at))
            at += group
    for jb, kb, source, at in pieces:
        for start in range(0, rows, pack):
            many = min(pack, rows - start)
            block = source[0, start * JB : (start + many) * JB, at : at + group].astype(
                jnp.float32
            )
            turned = -jnp.transpose(block) if jb != kb else None
            for n in range(many):
                for p in range(moments):
                    which = (start + n) * moments + p
                    for r in range(2):
                        lane = (2 * p + r) * JB
                        tile, spot = divmod(r * nvec + kb * JB, LANES)
                        full[
                            which * tall + tile, jb * JB : (jb + 1) * JB, spot : spot + JB
                        ] = block[n * JB : (n + 1) * JB, lane : lane + JB]
                        if jb != kb:
                            tile, spot = divmod(r * nvec + jb * JB, LANES)
                            full[
                                which * tall + tile, kb * JB : (kb + 1) * JB, spot : spot + JB
                            ] = turned[lane : lane + JB, n * JB : (n + 1) * JB]
    wide = 2 * nvec
    tiles = 2 * wide // LANES
    half = nvec // 2
    for which in range(rows * moments):
        parity = []
        for odd in range(2):
            for tile in range(tall):
                line = full[which * tall + tile, pl.ds(odd, half, stride=2), :]
                parity.append(line[:, : min(LANES, wide - tile * LANES)])
        both = jnp.concatenate(parity, axis=1)
        i, p = which // moments, which % moments
        base = i * half * tiles * moments
        for tile in range(tiles):
            out_ref[0, pl.ds(base + tile * moments + p, half, stride=tiles * moments), :] = both[
                :, tile * LANES : (tile + 1) * LANES
            ]


def unpack(head, tail, rows, moments, nvec):
    times = head.shape[0]
    lines = nvec * nvec * 2 // LANES
    flat = pl.pallas_call(
        functools.partial(unpack_kernel, rows, moments, nvec),
        out_shape=jax.ShapeDtypeStruct((times, rows * lines * moments, LANES), jnp.float32),
        grid=(times,),
        in_specs=[
            pl.BlockSpec((1,) + head.shape[1:], lambda t: (t, 0, 0)),
            pl.BlockSpec((1,) + tail.shape[1:], lambda t: (t, 0, 0)),
        ],
        out_specs=pl.BlockSpec((1, rows * lines * moments, LANES), lambda t: (t, 0, 0)),
        scratch_shapes=[
            pltpu.VMEM((rows * moments * -(-2 * nvec // LANES), nvec, LANES), jnp.float32)
        ],
        compiler_params=pltpu.CompilerParams(dimension_semantics=("arbitrary",)),
        name="unpack",
    )(head, tail)
    flat = flat.reshape(times, rows, lines, moments, LANES)
    return jnp.transpose(flat, (0, 1, 3, 2, 4)).reshape(times, rows, moments, lines * LANES)


def body(vectors, momenta, offsets):
    local = vectors[0]
    nvec = local.shape[2]
    sites = local.shape[3]
    groups = lax.axis_size("space")
    rows = nvec // groups
    moments = momenta.shape[0]
    nblocks = nvec // JB
    group = 2 * moments * JB
    mine = lax.axis_index("space") * rows
    half = sites // 2
    site_ids = jnp.arange(sites, dtype=jnp.int32)
    coords = local_coords(site_ids)[:, None, :] + jnp.transpose(offsets)[:, :, None]
    phase = phases(momenta, coords.reshape(3, groups * sites))
    phase = jnp.transpose(phase.reshape(2 * moments, groups, sites), (1, 0, 2))
    scale = 1.0 / math.sqrt(sites * groups)
    early = lax.all_gather(local[..., :half], "space", axis=0)
    late = lax.all_gather(local[..., half:], "space", axis=0)
    early_rows = lax.dynamic_slice_in_dim(early, mine, rows, 3)
    partial = contract(early, early_rows, phase[..., :half], scale, 0, nblocks, None, 0)
    late, partial = lax.optimization_barrier((late, partial))
    late_rows = lax.dynamic_slice_in_dim(late, mine, rows, 3)
    stage = (late, late_rows, phase[..., half:])
    cut = nblocks * group
    seeds = [(partial, 0), (partial, 1)]
    if 2 * cut != partial.shape[1]:
        seeds = [(partial[:, :cut], 0), (partial[:, cut:], 0)]
    head = contract(*stage, scale, 0, 1, *seeds[0])
    head = lax.all_gather(head, "tm", axis=0)
    tail = contract(*stage, scale, 1, nblocks, *seeds[1])
    tail = lax.all_gather(tail, "tm", axis=0)
    return unpack(head, tail, rows, moments, nvec)


def solution(mesh):
    return jax.shard_map(
        body,
        mesh=mesh,
        in_specs=(P("tm", None, None, None, "space"), P(), P()),
        out_specs=P(None, "space", None, None),
        check_vma=False,
    )
```
